32 devices in a mesh: tok: 8 (over z, x), mp: 4 (over y, core).
Axes of the slice: x: 2, y: 2, z: 4, core: 2. Of those that a mesh axis runs over, the one named last changes fastest.
Arguments:
- tokens: bfloat16 [3072, 2048], P('tok', 'mp'), may hold values from -120 to 120
- norm_gain: float32 [2048], replicated, may hold values from 0.5 to 1.5
- running_sq: float32 [2048], P('mp'), may hold values from 0.5 to 4
- gate_weight: bfloat16 [2048, 8192], P(None, 'mp'), may hold values from -0.125 to 0.125
- up_weight: bfloat16 [2048, 8192], P(None, 'mp'), may hold values from -0.125 to 0.125
- down_weight_t: bfloat16 [2048, 8192], P(None, 'mp'), may hold values from -0.0625 to 0.0625
- groups: int32 [192], P('tok'), may hold values from 0 to 23, as said below
- cotangent: bfloat16 [3072, 2048], P('tok', 'mp'), may hold values from -6 to 6
Outputs:
- block_out: bfloat16 [3072, 2048], P('tok', 'mp')
- grad_tokens: bfloat16 [3072, 2048], P('tok', 'mp')
- running_new: float32 [2048], P('mp')
- grad_gain: float32 [2048], P('mp')
- grad_gate: float32 [2048, 8192], P('tok', 'mp')
- grad_up: float32 [2048, 8192], P('tok', 'mp')
- grad_down_t: float32 [2048, 8192], P('tok', 'mp')
The draws below stay inside these ranges and needn't reach their ends.
Inputs may be any that keep to these rules, and one draw needn't show every extreme that they name: Each of the 24 ghost groups holds exactly 8 blocks.
All inputs are finite; a program needn't handle non-finite values.
Results may differ from the reference program's by a relative error of at most 0.02.
Values may be sent and summed in bfloat16 or wider, within the bound.
A program may use at most 128 MiB of HBM per device.

```python
import math
import jax
import jax.numpy as jnp
from jax import lax

D = 2048
FF = 8192
GHOST = 128
BLK = 16
TOKENS = 3072
GROUPS = 24
NBLK = 192


def draw_groups(key, part):
    blocks_per_group = GHOST // BLK
    order = jax.random.permutation(jax.random.fold_in(key, 11), NBLK)
    return (order // blocks_per_group).astype(jnp.int32)


def draw_tokens(key, part):
    key_base, key_block, key_column = jax.random.split(jax.random.fold_in(key, 23), 3)
    position = jnp.arange(TOKENS, dtype=jnp.float32)
    rising = jnp.exp(jnp.log(3.0) * position / TOKENS)
    block_scale = jnp.exp(jax.random.uniform(key_block, (NBLK,), jnp.float32, jnp.log(0.5), jnp.log(2.0)))
    row_scale = jnp.broadcast_to(block_scale[:, None], (NBLK, BLK)).reshape(TOKENS) * rising
    column_scale = jnp.exp(jax.random.uniform(key_column, (D,), jnp.float32, jnp.log(0.3), jnp.log(3.0)))
    base = jnp.clip(jax.random.normal(key_base, (TOKENS, D), jnp.float32), -6.0, 6.0)
    return (base * row_scale[:, None] * column_scale[None, :]).astype(jnp.bfloat16)


def level_of(stream_key, dims, pieces, low, top_value):
    def one(dim, shards_of):
        draws = jax.random.uniform(jax.random.fold_in(jax.random.fold_in(stream_key, 6), dim), (shards_of,), jnp.float32, low / len(pieces), top_value / len(pieces))
        return jnp.repeat(jnp.exp(draws), dims[dim] // shards_of).reshape((-1,) + (1,) * (len(dims) - dim - 1))

    loudness = one(*pieces[0])
    for cut in pieces[1:]:
        loudness = loudness * one(*cut)
    return loudness


def noise(rng, extent, width, bound, shards=(), kind=jnp.bfloat16):
    array = jax.random.normal(rng, extent, jnp.float32) * width
    if len(shards) > 0:
        array = level_of(rng, extent, shards, -0.22, 0.18) * array
    return jnp.clip(array, min=-bound, max=bound).astype(kind)


def setup_inputs(seed: int = 0) -> dict:
    key_of = jax.random.split(jax.random.key(seed), 9)
    return {
        "tokens": draw_tokens(jax.random.fold_in(key_of[8], 71), 0),
        "norm_gain": jnp.clip(1.0 + 0.1 * jax.random.normal(key_of[1], (D,), jnp.float32), 0.5, 1.5),
        "running_sq": jnp.clip(jnp.exp(math.log(4.0) - 2.0794415 * jax.random.uniform(key_of[2], (D,), jnp.float32) ** level_of(key_of[2], (D,), ((0, 4),), -0.2, 0.2)), 0.5, 4.0),
        "gate_weight": noise(key_of[3], (D, FF), D ** -0.5, 0.125, ((1, 4),)),
        "up_weight": noise(key_of[4], (D, FF), D ** -0.5, 0.125, ((1, 4),)),
        "down_weight_t": noise(key_of[5], (D, FF), FF ** -0.5, 0.0625, ((1, 4),)),
        "groups": draw_groups(jax.random.fold_in(key_of[8], 71), 0),
        "cotangent": noise(key_of[7], (TOKENS, D), 1.0, 6.0, ((0, 8), (1, 4))),
    }


epsilon = 1e-05
momentum = 0.1
highest = lax.Precision.HIGHEST

def group_onehot(groups):
    return (groups[None, :] == jnp.arange(GROUPS, dtype=jnp.int32)[:, None]).astype(jnp.float32)

def group_sums(values, onehot):
    blocks = values.reshape(values.shape[0] // BLK, BLK, values.shape[1]).sum(axis=1)
    return jnp.dot(onehot, blocks, precision=highest, preferred_element_type=jnp.float32)

def per_token(table, onehot):
    per_block = jnp.dot(onehot.T, table, precision=highest, preferred_element_type=jnp.float32)
    wide = jnp.broadcast_to(per_block[:, None, :], (per_block.shape[0], BLK, per_block.shape[1]))
    return wide.reshape(per_block.shape[0] * BLK, per_block.shape[1])

def reference(tokens, norm_gain, running_sq, gate_weight, up_weight, down_weight_t, groups, cotangent):
    onehot = group_onehot(groups)
    x_float = tokens.astype(jnp.float32)
    quad_mean = group_sums(x_float * x_float, onehot) / GHOST
    scale = per_token(lax.rsqrt(quad_mean + epsilon), onehot)
    normed = x_float * scale
    hid_in = (norm_gain * normed).astype(jnp.bfloat16)
    gate = jnp.dot(hid_in, gate_weight, preferred_element_type=jnp.float32)
    lift = jnp.dot(hid_in, up_weight, preferred_element_type=jnp.float32)
    sigma = jax.nn.sigmoid(gate)
    hidden = (gate * sigma * lift).astype(jnp.bfloat16)
    branch = lax.dot_general(hidden, down_weight_t, (((1,), (1,)), ((), ())), preferred_element_type=jnp.float32)
    block_out = (x_float + branch).astype(jnp.bfloat16)
    running_new = (1.0 - momentum) * running_sq + momentum * lax.optimization_barrier(jnp.mean(quad_mean, axis=0))
    grad_down_t = lax.dot_general(cotangent, hidden, (((0,), (0,)), ((), ())), preferred_element_type=jnp.float32)
    grad_hidden = jnp.dot(cotangent, down_weight_t, preferred_element_type=jnp.float32)
    grad_gate_in = (grad_hidden * lift * sigma * (1.0 + gate * (1.0 - sigma))).astype(jnp.bfloat16)
    grad_lift = (grad_hidden * gate * sigma).astype(jnp.bfloat16)
    grad_gate = lax.dot_general(hid_in, grad_gate_in, (((0,), (0,)), ((), ())), preferred_element_type=jnp.float32)
    grad_up = lax.dot_general(hid_in, grad_lift, (((0,), (0,)), ((), ())), preferred_element_type=jnp.float32)
    grad_normed_in = lax.dot_general(grad_gate_in, gate_weight, (((1,), (1,)), ((), ())), preferred_element_type=jnp.float32)
    grad_normed_in = grad_normed_in + lax.dot_general(grad_lift, up_weight, (((1,), (1,)), ((), ())), preferred_element_type=jnp.float32)
    partial_value = group_sums(grad_normed_in * normed, onehot)
    grad_gain = lax.optimization_barrier(jnp.sum(partial_value, axis=0))
    mean_term = per_token(norm_gain * partial_value / GHOST, onehot)
    grad_tokens = (cotangent.astype(jnp.float32) + scale * (norm_gain * grad_normed_in - normed * mean_term)).astype(jnp.bfloat16)
    return (block_out, grad_tokens, running_new, grad_gain, grad_gate, grad_up, grad_down_t)
```

```python
import jax
import jax.numpy as jnp
from jax import lax
from jax.sharding import PartitionSpec as P

GHOST = 128
BLK = 16


epsilon = 1e-05
momentum = 0.1
highest = lax.Precision.HIGHEST


def group_sums(values, onehot):
    blocks = values.reshape(values.shape[0] // BLK, BLK, values.shape[1]).sum(axis=1)
    return jnp.dot(onehot, blocks, precision=highest, preferred_element_type=jnp.float32)


def per_token(table, onehot):
    per_block = jnp.dot(onehot.T, table, precision=highest, preferred_element_type=jnp.float32)
    wide = jnp.broadcast_to(per_block[:, None, :], (per_block.shape[0], BLK, per_block.shape[1]))
    return wide.reshape(per_block.shape[0] * BLK, per_block.shape[1])


def contract_rows(left, right):
    return lax.dot_general(
        left, right, (((0,), (0,)), ((), ())), preferred_element_type=jnp.float32
    )


def contract_cols(left, right):
    return lax.dot_general(
        left, right, (((1,), (1,)), ((), ())), preferred_element_type=jnp.float32
    )


def swap(value, bit):
    count = lax.axis_size("tok")
    return lax.ppermute(value, "tok", [(i, i ^ bit) for i in range(count)])


def gather_stepwise(value, tie):
    bit = lax.axis_size("mp") // 2
    me = lax.axis_index("mp")
    rows, width = value.shape
    steps = 0
    while bit:
        arrived = lax.ppermute(
            value, "mp", [(i, i ^ bit) for i in range(lax.axis_size("mp"))]
        )
        if steps == 0:
            arrived = after(arrived, tie)
        upper = (me & bit) != 0
        value = jnp.stack([jnp.where(upper, arrived, value), jnp.where(upper, value, arrived)])
        steps += 1
        bit //= 2
    order = (steps,) + tuple(range(steps - 1, -1, -1)) + (steps + 1,)
    return value.transpose(order).reshape(rows, lax.axis_size("mp") * width)


def total_direct(value):
    count = lax.axis_size("tok")
    parts = [value] + [swap(value, mask) for mask in range(1, count)]
    while len(parts) > 1:
        parts = [parts[k] + parts[k + 1] for k in range(0, len(parts), 2)]
    return parts[0]


def after(values, earlier):
    return lax.optimization_barrier((values, earlier))[0]


def halve(terms, bit, onward=0, tie=None):
    for mask in sorted((m for m in terms if m & bit), reverse=True):
        arrived = swap(terms.pop(mask).astype(jnp.bfloat16), bit)
        if mask & onward:
            arrived = after(arrived, tie)
        merged = terms[mask ^ bit].astype(jnp.float32) + arrived.astype(jnp.float32)
        terms[mask ^ bit] = merged.astype(jnp.bfloat16) if mask & onward else merged
    return terms


def scatter_sum(terms, bits):
    for bit in bits:
        terms = halve(terms, bit)
    return terms[0]


def gather_mp(value):
    return lax.all_gather(value, "mp", axis=1, tiled=True)


def body(tokens, norm_gain, running_sq, gate_weight, up_weight, down_weight_t, groups, cotangent):
    tok_count = lax.axis_size("tok")
    me = lax.axis_index("tok")
    tok_rows, feat_width = tokens.shape
    groups_total = tok_rows * tok_count // GHOST
    pair_bit = tok_count // 2
    bits = [1 << k for k in range(tok_count.bit_length() - 2)]
    masks = range(pair_bit)

    onehot = (groups[None, :] == jnp.arange(groups_total, dtype=jnp.int32)[:, None]).astype(
        jnp.float32
    )
    col_first = lax.axis_index("mp") * feat_width
    x_local = tokens.astype(jnp.float32)
    gain_local = lax.dynamic_slice_in_dim(norm_gain, col_first, feat_width, 0)
    squares = group_sums(x_local * x_local, onehot)
    squares = squares + swap(squares, pair_bit)
    dy_local = after(cotangent, squares)
    dy_both = jnp.concatenate([dy_local, swap(dy_local, pair_bit)], axis=0)
    for bit in reversed(bits):
        squares = squares + swap(squares, bit)
    quad_mean = squares / GHOST
    scale = per_token(lax.rsqrt(quad_mean + epsilon), onehot)
    normed = x_local * scale
    hid_local = (gain_local * normed).astype(jnp.bfloat16)
    hid_in = gather_mp(hid_local)
    hid_pair = gather_mp(swap(hid_local, pair_bit))
    running_new = (1.0 - momentum) * running_sq + momentum * jnp.mean(quad_mean, axis=0)

    def hidden_side(hid):
        gate = jnp.dot(hid, gate_weight, preferred_element_type=jnp.float32)
        lift = jnp.dot(hid, up_weight, preferred_element_type=jnp.float32)
        return gate, lift, (gate * jax.nn.sigmoid(gate) * lift).astype(jnp.bfloat16)

    def gradient_side(dy, gate, lift):
        sigma = jax.nn.sigmoid(gate)
        grad_hidden = jnp.dot(dy, down_weight_t, preferred_element_type=jnp.float32)
        grad_gate_in = (grad_hidden * lift * sigma * (1.0 + gate * (1.0 - sigma))).astype(
            jnp.bfloat16
        )
        grad_lift = (grad_hidden * gate * sigma).astype(jnp.bfloat16)
        return grad_gate_in, grad_lift

    out_rows = hid_in.shape[1] // tok_count

    def row_terms(left, left_pair, right, right_pair, chosen, sent):
        terms = {}
        for mask in sorted(chosen, reverse=True):
            first = (me ^ mask) * out_rows
            mine = lax.dynamic_slice_in_dim(left, first, out_rows, 1)
            other = lax.dynamic_slice_in_dim(left_pair, first, out_rows, 1)
            terms[mask] = contract_rows(mine, right) + contract_rows(other, right_pair)
            if sent:
                terms[mask] = terms[mask].astype(jnp.bfloat16)
        return terms

    def split_masks(bit):
        return [m for m in masks if m & bit], [m for m in masks if not m & bit]

    low, high = bits[0], bits[-1]
    low_sent, low_kept = split_masks(low)
    high_sent, high_kept = split_masks(high)

    gate, lift, hidden = hidden_side(hid_in)
    dy_both = gather_stepwise(dy_both, hidden)
    dy_full, dy_pair = dy_both[:tok_rows], dy_both[tok_rows:]
    grad_gate_in, grad_lift = gradient_side(dy_full, gate, lift)
    gate_pair, lift_pair, hidden_pair = hidden_side(hid_pair)

    down_terms = row_terms(dy_full, dy_pair, hidden, hidden_pair, low_sent, True)
    dy_pair_late = after(dy_pair, down_terms)
    grad_gate_in_pair, grad_lift_pair = gradient_side(dy_pair_late, gate_pair, lift_pair)
    down_terms.update(row_terms(dy_full, dy_pair, hidden, hidden_pair, low_kept, False))

    gate_terms = row_terms(hid_in, hid_pair, grad_gate_in, grad_gate_in_pair, high_sent, True)
    lift_a, lift_pair_a = after((grad_lift, grad_lift_pair), gate_terms)
    up_terms = row_terms(hid_in, hid_pair, lift_a, lift_pair_a, low_sent, True)
    gate_terms.update(
        row_terms(hid_in, hid_pair, grad_gate_in, grad_gate_in_pair, high_kept, False)
    )
    down_half = halve(down_terms, low, high, gate_terms)
    onward = {mask: term for mask, term in down_half.items() if mask & high}
    gate_c, lift_c = after((grad_gate_in, lift_a), (up_terms, onward))
    grad_partial = (
        contract_cols(gate_c, gate_weight) + contract_cols(lift_c, up_weight)
    ).astype(jnp.bfloat16)
    lift_d, lift_pair_d = after((lift_a, lift_pair_a), grad_partial)
    up_terms.update(row_terms(hid_in, hid_pair, lift_d, lift_pair_d, low_kept, False))
    hidden_late = after(hidden, up_terms)

    grad_down_t = scatter_sum(down_half, bits[1:])
    grad_gate = scatter_sum(gate_terms, bits[::-1])
    grad_up = scatter_sum(up_terms, bits)

    branch = lax.psum_scatter(
        contract_cols(hidden_late, down_weight_t).astype(jnp.bfloat16),
        "mp",
        scatter_dimension=1,
        tiled=True,
    ).astype(jnp.float32)
    block_out = (x_local + branch).astype(jnp.bfloat16)
    grad_normed_in = lax.psum_scatter(
        grad_partial, "mp", scatter_dimension=1, tiled=True
    ).astype(jnp.float32)
    partial_value = total_direct(group_sums(grad_normed_in * normed, onehot))
    grad_gain = jnp.sum(partial_value, axis=0)
    mean_term = per_token(gain_local * partial_value / GHOST, onehot)
    grad_tokens = (
        cotangent.astype(jnp.float32) + scale * (gain_local * grad_normed_in - normed * mean_term)
    ).astype(jnp.bfloat16)
    return (block_out, grad_tokens, running_new, grad_gain, grad_gate, grad_up, grad_down_t)


def solution(mesh):
    placed = (
        P("tok", "mp"),
        P(),
        P("mp"),
        P(None, "mp"),
        P(None, "mp"),
        P(None, "mp"),
        P("tok"),
        P("tok", "mp"),
    )
    return jax.shard_map(
        body,
        mesh=mesh,
        in_specs=placed,
        out_specs=(
            P("tok", "mp"),
            P("tok", "mp"),
            P("mp"),
            P("mp"),
            P("tok", "mp"),
            P("tok", "mp"),
            P("tok", "mp"),
        ),
        check_vma=False,
    )
```

```python
import jax
import jax.numpy as jnp
from jax import lax
from jax.sharding import PartitionSpec as P

GHOST = 128
BLK = 16


epsilon = 1e-05
momentum = 0.1
highest = lax.Precision.HIGHEST


def group_sums(values, onehot):
    blocks = values.reshape(values.shape[0] // BLK, BLK, values.shape[1]).sum(axis=1)
    return jnp.dot(onehot, blocks, precision=highest, preferred_element_type=jnp.float32)


def per_token(table, onehot):
    per_block = jnp.dot(onehot.T, table, precision=highest, preferred_element_type=jnp.float32)
    wide = jnp.broadcast_to(per_block[:, None, :], (per_block.shape[0], BLK, per_block.shape[1]))
    return wide.reshape(per_block.shape[0] * BLK, per_block.shape[1])


def contract_rows(left, right):
    return lax.dot_general(
        left, right, (((0,), (0,)), ((), ())), preferred_element_type=jnp.float32
    )


def contract_cols(left, right):
    return lax.dot_general(
        left, right, (((1,), (1,)), ((), ())), preferred_element_type=jnp.float32
    )


def swap(value, bit):
    count = lax.axis_size("tok")
    return lax.ppermute(value, "tok", [(i, i ^ bit) for i in range(count)])


def gather_stepwise(value, tie=None):
    bit = lax.axis_size("mp") // 2
    me = lax.axis_index("mp")
    rows, width = value.shape
    steps = 0
    while bit:
        arrived = lax.ppermute(
            value, "mp", [(i, i ^ bit) for i in range(lax.axis_size("mp"))]
        )
        if tie is not None and bit == 1:
            arrived = after(arrived, tie)
        upper = (me & bit) != 0
        value = jnp.stack([jnp.where(upper, arrived, value), jnp.where(upper, value, arrived)])
        steps += 1
        bit //= 2
    order = (steps,) + tuple(range(steps - 1, -1, -1)) + (steps + 1,)
    return value.transpose(order).reshape(rows, lax.axis_size("mp") * width)


def total_direct(value):
    count = lax.axis_size("tok")
    parts = [value] + [swap(value, mask) for mask in range(1, count)]
    while len(parts) > 1:
        parts = [parts[k] + parts[k + 1] for k in range(0, len(parts), 2)]
    return parts[0]


def after(values, earlier):
    return lax.optimization_barrier((values, earlier))[0]


def halve(terms, bit, onward=0, tie=None):
    for mask in sorted((m for m in terms if m & bit), reverse=True):
        arrived = swap(terms.pop(mask).astype(jnp.bfloat16), bit)
        if mask & onward:
            arrived = after(arrived, tie)
        merged = terms[mask ^ bit].astype(jnp.float32) + arrived.astype(jnp.float32)
        terms[mask ^ bit] = merged.astype(jnp.bfloat16) if mask & onward else merged
    return terms


def scatter_sum(terms, bits):
    for bit in bits:
        terms = halve(terms, bit)
    return terms[0]


def gather_mp(value):
    return lax.all_gather(value, "mp", axis=1, tiled=True)


def body(tokens, norm_gain, running_sq, gate_weight, up_weight, down_weight_t, groups, cotangent):
    tok_count = lax.axis_size("tok")
    me = lax.axis_index("tok")
    tok_rows, feat_width = tokens.shape
    groups_total = tok_rows * tok_count // GHOST
    pair_bit = tok_count // 2
    bits = [1 << k for k in range(tok_count.bit_length() - 2)]
    masks = range(pair_bit)

    dy_pair_local = swap(cotangent, pair_bit)
    onehot = (groups[None, :] == jnp.arange(groups_total, dtype=jnp.int32)[:, None]).astype(
        jnp.float32
    )
    col_first = lax.axis_index("mp") * feat_width
    x_local = tokens.astype(jnp.float32)
    gain_local = lax.dynamic_slice_in_dim(norm_gain, col_first, feat_width, 0)
    squares = group_sums(x_local * x_local, onehot)
    for bit in bits + [pair_bit]:
        squares = squares + swap(squares, bit)
    quad_mean = squares / GHOST
    scale = per_token(lax.rsqrt(quad_mean + epsilon), onehot)
    normed = x_local * scale
    hid_local = (gain_local * normed).astype(jnp.bfloat16)
    hid_in = gather_mp(hid_local)
    hid_pair = gather_mp(swap(hid_local, pair_bit))
    running_new = (1.0 - momentum) * running_sq + momentum * jnp.mean(quad_mean, axis=0)

    def hidden_side(hid):
        gate = jnp.dot(hid, gate_weight, preferred_element_type=jnp.float32)
        lift = jnp.dot(hid, up_weight, preferred_element_type=jnp.float32)
        return gate, lift, (gate * jax.nn.sigmoid(gate) * lift).astype(jnp.bfloat16)

    def gradient_side(dy, gate, lift):
        sigma = jax.nn.sigmoid(gate)
        grad_hidden = jnp.dot(dy, down_weight_t, preferred_element_type=jnp.float32)
        grad_gate_in = (grad_hidden * lift * sigma * (1.0 + gate * (1.0 - sigma))).astype(
            jnp.bfloat16
        )
        grad_lift = (grad_hidden * gate * sigma).astype(jnp.bfloat16)
        return grad_gate_in, grad_lift

    out_rows = hid_in.shape[1] // tok_count

    def row_terms(left, left_pair, right, right_pair, chosen, sent):
        terms = {}
        for mask in sorted(chosen, reverse=True):
            first = (me ^ mask) * out_rows
            mine = lax.dynamic_slice_in_dim(left, first, out_rows, 1)
            other = lax.dynamic_slice_in_dim(left_pair, first, out_rows, 1)
            terms[mask] = contract_rows(mine, right) + contract_rows(other, right_pair)
            if sent:
                terms[mask] = terms[mask].astype(jnp.bfloat16)
        return terms

    def split_masks(bit):
        return [m for m in masks if m & bit], [m for m in masks if not m & bit]

    low, high = bits[0], bits[-1]
    low_sent, low_kept = split_masks(low)
    high_sent, high_kept = split_masks(high)

    gate, lift, hidden = hidden_side(hid_in)
    dy_full = gather_stepwise(cotangent, hidden)
    dy_pair = gather_stepwise(after(dy_pair_local, hidden))
    grad_gate_in, grad_lift = gradient_side(dy_full, gate, lift)
    gate_pair, lift_pair, hidden_pair = hidden_side(hid_pair)

    down_terms = row_terms(dy_full, dy_pair, hidden, hidden_pair, low_sent, True)
    dy_pair_late = after(dy_pair, down_terms)
    grad_gate_in_pair, grad_lift_pair = gradient_side(dy_pair_late, gate_pair, lift_pair)
    down_terms.update(row_terms(dy_full, dy_pair, hidden, hidden_pair, low_kept, False))

    gate_terms = row_terms(hid_in, hid_pair, grad_gate_in, grad_gate_in_pair, high_sent, True)
    lift_a, lift_pair_a = after((grad_lift, grad_lift_pair), gate_terms)
    up_terms = row_terms(hid_in, hid_pair, lift_a, lift_pair_a, low_sent, True)
    gate_terms.update(
        row_terms(hid_in, hid_pair, grad_gate_in, grad_gate_in_pair, high_kept, False)
    )
    down_half = halve(down_terms, low, high, gate_terms)
    onward = {mask: term for mask, term in down_half.items() if mask & high}
    gate_c, lift_c = after((grad_gate_in, lift_a), (up_terms, onward))
    grad_partial = (
        contract_cols(gate_c, gate_weight) + contract_cols(lift_c, up_weight)
    ).astype(jnp.bfloat16)
    lift_d, lift_pair_d = after((lift_a, lift_pair_a), grad_partial)
    up_terms.update(row_terms(hid_in, hid_pair, lift_d, lift_pair_d, low_kept, False))
    hidden_late = after(hidden, up_terms)

    grad_down_t = scatter_sum(down_half, bits[1:])
    grad_gate = scatter_sum(gate_terms, bits[::-1])
    grad_up = scatter_sum(up_terms, bits)

    branch = lax.psum_scatter(
        contract_cols(hidden_late, down_weight_t).astype(jnp.bfloat16),
        "mp",
        scatter_dimension=1,
        tiled=True,
    ).astype(jnp.float32)
    block_out = (x_local + branch).astype(jnp.bfloat16)
    grad_normed_in = lax.psum_scatter(
        grad_partial, "mp", scatter_dimension=1, tiled=True
    ).astype(jnp.float32)
    partial_value = total_direct(group_sums(grad_normed_in * normed, onehot))
    grad_gain = jnp.sum(partial_value, axis=0)
    mean_term = per_token(gain_local * partial_value / GHOST, onehot)
    grad_tokens = (
        cotangent.astype(jnp.float32) + scale * (gain_local * grad_normed_in - normed * mean_term)
    ).astype(jnp.bfloat16)
    return (block_out, grad_tokens, running_new, grad_gain, grad_gate, grad_up, grad_down_t)


def solution(mesh):
    placed = (
        P("tok", "mp"),
        P(),
        P("mp"),
        P(None, "mp"),
        P(None, "mp"),
        P(None, "mp"),
        P("tok"),
        P("tok", "mp"),
    )
    return jax.shard_map(
        body,
        mesh=mesh,
        in_specs=placed,
        out_specs=(
            P("tok", "mp"),
            P("tok", "mp"),
            P("mp"),
            P("mp"),
            P("tok", "mp"),
            P("tok", "mp"),
            P("tok", "mp"),
        ),
        check_vma=False,
    )
```
